32 devices in a mesh: section: 4 (over y, x), cp: 4 (over z), tp: 2 (over core).
Axes of the slice: x: 2, y: 2, z: 4, core: 2. Of those that a mesh axis runs over, the one named last changes fastest.
Arguments:
- acts: bfloat16 [4, 512, 8192], P('section', 'cp', 'tp'), may hold values from -16 to 16
- keys: bfloat16 [4, 512, 1024], P('section', 'cp', 'tp'), may hold values from -4 to 4
- values: bfloat16 [4, 512, 1024], P('section', 'cp', 'tp'), may hold values from -6 to 6
- grads: bfloat16 [4, 512, 8192], P('section', 'cp', 'tp'), may hold values from -6 to 6
- docs: int32 [4, 512], P('section'), may hold values from 0 to 7, never falling along the last dimension, each value on 1 to 256 neighbouring positions
- order: int32 [4, 512], P('section'), may hold values from 0 to 511, each once within a row
Outputs:
- outputs: bfloat16 [4, 512, 8192], P('section', 'cp', 'tp')
- grad_query: bfloat16 [4, 512, 8192], P('section', 'cp', 'tp')
- grad_keys: bfloat16 [4, 512, 1024], P('section', 'cp', 'tp')
- grad_values: bfloat16 [4, 512, 1024], P('section', 'cp', 'tp')
The draws below stay inside these ranges and needn't reach their ends.
Inputs may be any that keep to these rules, and one draw needn't show every extreme that they name: `docs`: along positions of one section the document numbers never fall; each document holds 1 to 256 tokens. `order`: each section's row holds every position once.
All inputs are finite; a program needn't handle non-finite values.
Results may differ from the reference program's by a relative error of at most 0.0061.
Values may be sent and summed in bfloat16 or wider, within the bound.
A program may use at most 64 MiB of HBM per device.

```python
import math
import jax
import jax.numpy as jnp
import numpy as np
from jax import lax

HEADS = 64
KV_HEADS = 8
HEAD = 128
DOCS = 8
TOKENS = 512
SECTIONS = 4
DOC_MOST = 256
QW = 8192
KVW = 1024


def draw_acts(key, part):
    shape = (SECTIONS, TOKENS, HEADS * HEAD)
    result = jax.random.truncated_normal(jax.random.fold_in(key, 11), -4.0, 4.0, shape, jnp.float32)
    return result.astype(jnp.bfloat16)


def draw_keys(key, part):
    shape = (SECTIONS, TOKENS, KV_HEADS * HEAD)
    result = jax.random.truncated_normal(jax.random.fold_in(key, 13), -4.0, 4.0, shape, jnp.float32)
    return result.astype(jnp.bfloat16)


def block_levels(key, shape, split, least, largest):
    level = 1.0
    for dim, shards_of in split:
        steps = jax.random.uniform(jax.random.fold_in(jax.random.fold_in(key, 6), dim), (shards_of,), jnp.float32, least / len(split), largest / len(split))
        level = level * jnp.repeat(jnp.exp(steps), shape[dim] // shards_of).reshape((-1,) + (1,) * (len(shape) - 1 - dim))
    return level


def split_up(amount, total, reach, skew):
    weights = [(1 << 20) // math.isqrt(grade ** skew) + 1 for grade in range(2, amount + 1)]
    rest, counts = total - reach - (amount - 1), [1] * (amount - 1)
    while rest > 0:
        movable = [i for i in range(amount - 1) if counts[i] < reach]
        mass, left = sum([weights[i] for i in movable]), rest
        for i in movable:
            more = min(reach - counts[i], max(1, left * weights[i] // mass), rest)
            counts[i] = counts[i] + more
            rest = rest - more
    return np.array([reach] + counts)


def ragged(stream_key, count, total, limit, skew):
    if count == 2:
        one = jax.random.randint(stream_key, (), max(1, total - limit), min(limit, total - 1) + 1)
        return jnp.stack([one, total - one])
    sizes = jnp.asarray(split_up(count, total, limit, skew), jnp.int32)
    couples = (count - 1) // 2
    source_of, receiver = sizes[1:1 + 2 * couples:2], sizes[2:2 + 2 * couples:2]
    slack = jnp.minimum(source_of - 1, limit - receiver)
    shifted = jax.random.randint(jax.random.fold_in(stream_key, 1), (couples,), 0, 1 << 20) % (slack + 1)
    sizes = sizes.at[1:1 + 2 * couples:2].set(source_of - shifted).at[2:2 + 2 * couples:2].set(receiver + shifted)
    return sizes[jax.random.permutation(jax.random.fold_in(stream_key, 2), count)]


def bell_draw(own_key, shape, width, limit, shards=(), held_as=jnp.bfloat16):
    loudness = block_levels(own_key, shape, shards, -0.22, 0.18) if shards else 1.0
    entries = jax.random.normal(own_key, shape, jnp.float32) * width * loudness
    return jnp.minimum(jnp.maximum(entries, -limit), limit).astype(held_as)


def setup_inputs(seed: int = 0) -> dict:
    seeds = jax.random.split(jax.random.key(seed), 7)
    acts = draw_acts(jax.random.fold_in(seeds[6], 71), 0)
    keys = draw_keys(jax.random.fold_in(seeds[6], 71), 0)
    values = bell_draw(seeds[2], (SECTIONS, TOKENS, KVW), 1.0, 6.0, ((0, 4), (1, 4), (2, 2)))
    grads = bell_draw(seeds[3], (SECTIONS, TOKENS, QW), 1.0, 6.0, ((0, 4), (1, 4), (2, 2)))
    docs = jax.vmap(lambda own: jnp.searchsorted(jnp.cumsum(ragged(own, DOCS, TOKENS, DOC_MOST, 1)), jnp.arange(TOKENS), side="right"))(jax.random.split(seeds[4], SECTIONS)).reshape((SECTIONS, TOKENS)).astype(jnp.int32)
    order = jax.vmap(lambda own: jax.random.permutation(own, TOKENS))(jax.random.split(seeds[5], SECTIONS)).reshape((SECTIONS, TOKENS)).astype(jnp.int32)
    return {"acts": acts, "keys": keys, "values": values, "grads": grads, "docs": docs, "order": order}


def split_heads(block, kv_count):
    tokens = block.shape[0]
    group = block.shape[1] // (kv_count * HEAD)
    return block.reshape(tokens, kv_count, group, HEAD).transpose(1, 2, 0, 3).reshape(kv_count, group * tokens, HEAD)


def join_heads(rows, tokens):
    kv_count = rows.shape[0]
    group = rows.shape[1] // tokens
    return rows.reshape(kv_count, group, tokens, HEAD).transpose(2, 0, 1, 3).reshape(tokens, kv_count * group * HEAD)


def forward_part(flat_q, key, value, allowed):
    scale = HEAD ** -0.5
    rows_q = allowed.shape[0]
    scores = lax.dot_general(flat_q, key, (((1,), (1,)), ((), ())), preferred_element_type=jnp.float32) * scale
    scores = scores.reshape(-1, rows_q, key.shape[0])
    scores = jnp.where(allowed[None], scores, -jnp.inf)
    peak = jnp.max(scores, axis=2, keepdims=True)
    expd = jnp.exp(scores - peak)
    probs = (expd / jnp.sum(expd, axis=2, keepdims=True)).astype(jnp.bfloat16)
    probs = probs.reshape(flat_q.shape[0], key.shape[0])
    attended = jnp.dot(probs, value, preferred_element_type=jnp.float32)
    return probs, attended


def backward_part(probs, attended, flat_g, key, value):
    scale = HEAD ** -0.5
    delta = jnp.sum(flat_g.astype(jnp.float32) * attended, axis=1, keepdims=True)
    dprob = lax.dot_general(flat_g, value, (((1,), (1,)), ((), ())), preferred_element_type=jnp.float32)
    dscore = (probs.astype(jnp.float32) * (dprob - delta)).astype(jnp.bfloat16)
    dquery = jnp.dot(dscore, key, preferred_element_type=jnp.float32) * scale
    return dscore, dquery


def key_terms(probs, dscore, flat_q, flat_g):
    scale = HEAD ** -0.5
    dkey = lax.dot_general(dscore, flat_q, (((0,), (0,)), ((), ())), preferred_element_type=jnp.float32) * scale
    dvalue = lax.dot_general(probs, flat_g, (((0,), (0,)), ((), ())), preferred_element_type=jnp.float32)
    return dkey, dvalue


def section_pass(items):
    query, key, value, cotan, doc_row, order_row = items
    tokens = query.shape[0]
    kv_count = key.shape[1] // HEAD
    doc_all = jnp.take(doc_row, order_row)
    allowed = (doc_all[:, None] == doc_all[None, :]) & (order_row[None, :] <= order_row[:, None])
    q_rows = split_heads(query, kv_count)
    g_rows = split_heads(cotan, kv_count)
    k_heads = key.reshape(tokens, kv_count, HEAD).transpose(1, 0, 2)
    v_heads = value.reshape(tokens, kv_count, HEAD).transpose(1, 0, 2)

    def one_head(parts):
        probs, attended = forward_part(parts[0], parts[1], parts[2], allowed)
        dscore, dquery = backward_part(probs, attended, parts[3], parts[1], parts[2])
        dkey, dvalue = key_terms(probs, dscore, parts[0], parts[3])
        return attended, dquery, dkey, dvalue

    attended, dqueries, dkeys, dvalues = lax.map(one_head, (q_rows, k_heads, v_heads, g_rows))
    outputs = (query.astype(jnp.float32) + join_heads(attended, tokens)).astype(jnp.bfloat16)
    grad_query = (cotan.astype(jnp.float32) + join_heads(dqueries, tokens)).astype(jnp.bfloat16)
    grad_keys = dkeys.transpose(1, 0, 2).reshape(tokens, kv_count * HEAD).astype(jnp.bfloat16)
    grad_values = dvalues.transpose(1, 0, 2).reshape(tokens, kv_count * HEAD).astype(jnp.bfloat16)
    return outputs, grad_query, grad_keys, grad_values


def reference(acts, keys, values, grads, docs, order):
    arriving = jnp.roll(acts, 1, axis=0)
    returning = jnp.roll(grads, -1, axis=0)
    outputs, grad_query, grad_keys, grad_values = lax.map(section_pass, (arriving, keys, values, returning, docs, order))
    return (outputs, grad_query, grad_keys, grad_values)
```

```python
import functools

import jax
import jax.numpy as jnp
from jax import lax
from jax.experimental import pallas as pl
from jax.experimental.pallas import tpu as pltpu
from jax.sharding import PartitionSpec as P

HEAD = 128
DOCS = 8
MESH = pl.DeviceIdType.MESH


def times(a, b, dims):
    return lax.dot_general(a, b, (dims, ((), ())), preferred_element_type=jnp.float32)


def relay_kernel(
    heads, packs, pack, sections, blocks,
    acts, keys, values, grads, docs, order,
    out, gq, gk, gv,
    qbuf, gbuf, kbuf, vbuf, kt, vt, bias, dk, dv, terms, met,
    sec_send, sec_recv, kv_send, kv_recv, own_sem, red_send, red_recv,
):
    scale = HEAD ** (-0.5)
    tok = qbuf.shape[1]
    wide_cols = pack * HEAD
    section = lax.axis_index("section")
    me = lax.axis_index("cp")
    after = lax.rem(section + 1, sections)
    before = lax.rem(section + sections - 1, sections)

    def peer(off):
        return lax.rem(me + off, blocks)

    barrier = pltpu.get_barrier_semaphore()
    for where in (after, before):
        pl.semaphore_signal(barrier, inc=1, device_id={"section": where}, device_id_type=MESH)
    for off in range(1, blocks):
        pl.semaphore_signal(barrier, inc=1, device_id={"cp": peer(off)}, device_id_type=MESH)
    pl.semaphore_wait(barrier, 1 + blocks)

    def moved(step, which):
        src, dst, where = ((acts, qbuf, after), (grads, gbuf, before))[which]
        cols = pl.ds(pl.multiple_of(step * wide_cols, wide_cols), wide_cols)
        return pltpu.make_async_remote_copy(
            src_ref=src.at[0, :, cols],
            dst_ref=dst.at[step],
            send_sem=sec_send.at[step, which],
            recv_sem=sec_recv.at[step, which],
            device_id={"section": where},
            device_id_type=MESH,
        )

    def mine(ref, head):
        cols = pl.ds(pl.multiple_of(head * HEAD, HEAD), HEAD)
        return ref.at[0, :, cols]

    own_rows = pl.ds(pl.multiple_of(me * tok, tok), tok)

    def shared(head, which, off):
        src, dst = ((keys, kbuf), (values, vbuf))[which]
        return pltpu.make_async_remote_copy(
            src_ref=mine(src, head),
            dst_ref=dst.at[head, own_rows],
            send_sem=kv_send.at[head, which, off - 1],
            recv_sem=kv_recv.at[head, which, off - 1],
            device_id={"cp": peer(off)},
            device_id_type=MESH,
        )

    def kept(head, which):
        src, dst = ((keys, kbuf), (values, vbuf))[which]
        return pltpu.make_async_copy(
            mine(src, head), dst.at[head, own_rows], own_sem.at[head, which]
        )

    def returned(head, off):
        rows = pl.ds(pl.multiple_of(peer(off) * tok, tok), tok)
        return pltpu.make_async_remote_copy(
            src_ref=terms.at[head, rows],
            dst_ref=met.at[head, off - 1],
            send_sem=red_send.at[head, off - 1],
            recv_sem=red_recv.at[head, off - 1],
            device_id={"cp": peer(off)},
            device_id_type=MESH,
        )

    @pl.loop(0, heads)
    def _(head):
        @pl.loop(0, packs)
        def _(p):
            for which in range(2):
                moved(head * packs + p, which).start()

        for which in range(2):
            for off in range(1, blocks):
                shared(head, which, off).start()
            kept(head, which).start()

    positions = order[...].astype(jnp.float32)
    asked = order[:, own_rows].astype(jnp.float32)
    low = jnp.zeros_like(asked)
    for doc in range(1, DOCS):
        start = jnp.sum(
            jnp.where(docs[...] < doc, 1.0, 0.0), axis=1, keepdims=True
        )
        low = jnp.maximum(low, jnp.where(start <= asked, start, 0.0))
    count = positions.shape[1]
    stored = jnp.broadcast_to(positions, (tok, count)).T
    allowed = (stored <= asked) & (stored >= low)
    bias[...] = jnp.where(allowed, 0.0, -1e30)

    def finish(head):
        total = terms[head, own_rows, :].astype(jnp.float32)
        for off in range(1, blocks):
            returned(head, off).wait_recv()
            total = total + met[head, off - 1].astype(jnp.float32)
        cols = pl.ds(pl.multiple_of(head * HEAD, HEAD), HEAD)
        gk[0, :, cols] = total[:, :HEAD].astype(jnp.bfloat16)
        gv[0, :, cols] = total[:, HEAD:].astype(jnp.bfloat16)

    @pl.loop(0, heads)
    def _(head):
        for which in range(2):
            kept(head, which).wait()
            for off in range(1, blocks):
                shared(head, which, off).wait_recv()
        kt[...] = kbuf[head].T
        vt[...] = vbuf[head].T
        dk[...] = jnp.zeros_like(dk)
        dv[...] = jnp.zeros_like(dv)

        @pl.loop(0, packs)
        def _(p):
            step = head * packs + p
            for which in range(2):
                moved(step, which).wait_recv()
            parts = [slice(j * HEAD, (j + 1) * HEAD) for j in range(pack)]
            q = jnp.concatenate([qbuf[step, :, c] for c in parts], axis=0)
            g = jnp.concatenate([gbuf[step, :, c] for c in parts], axis=0)
            masked = jnp.concatenate([bias[...]] * pack, axis=1)
            k, v = kbuf[head], vbuf[head]
            scores = times(k, q, ((1,), (1,))) * scale + masked
            expd = jnp.exp(scores - jnp.max(scores, axis=0, keepdims=True))
            probs = (expd * (1.0 / jnp.sum(expd, axis=0, keepdims=True))).astype(jnp.bfloat16)
            attended = times(vt[...], probs, ((1,), (0,))).T
            dprob = times(v, g, ((1,), (1,)))
            wide = probs.astype(jnp.float32)
            delta = jnp.sum(wide * dprob, axis=0, keepdims=True)
            dscore = (wide * (dprob - delta)).astype(jnp.bfloat16)
            dquery = times(kt[...], dscore, ((1,), (0,))).T
            full = (q.astype(jnp.float32) + attended).astype(jnp.bfloat16)
            grad = (g.astype(jnp.float32) + dquery * scale).astype(jnp.bfloat16)
            for j in range(pack):
                cols = pl.ds(pl.multiple_of(step * wide_cols + j * HEAD, HEAD), HEAD)
                out[0, :, cols] = full[j * tok : (j + 1) * tok]
                gq[0, :, cols] = grad[j * tok : (j + 1) * tok]
            dk[...] += times(dscore, q, ((1,), (0,)))
            dv[...] += times(probs, g, ((1,), (0,)))

        terms[head, :, :HEAD] = (dk[...] * scale).astype(jnp.bfloat16)
        terms[head, :, HEAD:] = dv[...].astype(jnp.bfloat16)
        for off in range(1, blocks):
            returned(head, off).start()

        @pl.when(head > 0)
        def _():
            finish(head - 1)

    finish(heads - 1)

    @pl.loop(0, heads)
    def _(head):
        @pl.loop(0, packs)
        def _(p):
            for which in range(2):
                moved(head * packs + p, which).wait_send()

        for off in range(1, blocks):
            for which in range(2):
                shared(head, which, off).wait_send()
            returned(head, off).wait_send()


def on_device(acts, keys, values, grads, docs, order):
    tok = acts.shape[1]
    heads = keys.shape[2] // HEAD
    group = acts.shape[2] // keys.shape[2]
    pack = 2 if group % 2 == 0 else 1
    packs = group // pack
    sections, blocks = lax.axis_size("section"), lax.axis_size("cp")
    count = blocks * tok
    steps = heads * packs
    pairs = group * heads * tok * count
    half, dma = jnp.bfloat16, pltpu.SemaphoreType.DMA
    far = pl.BlockSpec(memory_space=pl.ANY)
    near = pl.BlockSpec(memory_space=pltpu.VMEM)
    return pl.pallas_call(
        functools.partial(relay_kernel, heads, packs, pack, sections, blocks),
        out_shape=(
            jax.ShapeDtypeStruct(acts.shape, half),
            jax.ShapeDtypeStruct(acts.shape, half),
            jax.ShapeDtypeStruct(keys.shape, half),
            jax.ShapeDtypeStruct(keys.shape, half),
        ),
        in_specs=[far] * 4 + [near] * 2,
        out_specs=(near,) * 4,
        scratch_shapes=[
            pltpu.VMEM((steps, tok, pack * HEAD), half),
            pltpu.VMEM((steps, tok, pack * HEAD), half),
            pltpu.VMEM((heads, count, HEAD), half),
            pltpu.VMEM((heads, count, HEAD), half),
            pltpu.VMEM((HEAD, count), half),
            pltpu.VMEM((HEAD, count), half),
            pltpu.VMEM((count, tok), jnp.float32),
            pltpu.VMEM((count, HEAD), jnp.float32),
            pltpu.VMEM((count, HEAD), jnp.float32),
            pltpu.VMEM((heads, count, 2 * HEAD), half),
            pltpu.VMEM((heads, blocks - 1, tok, 2 * HEAD), half),
            dma((steps, 2)),
            dma((steps, 2)),
            dma((heads, 2, blocks - 1)),
            dma((heads, 2, blocks - 1)),
            dma((heads, 2)),
            dma((heads, blocks - 1)),
            dma((heads, blocks - 1)),
        ],
        compiler_params=pltpu.CompilerParams(
            collective_id=0,
            has_side_effects=True,
            vmem_limit_bytes=48 * 1024 * 1024,
        ),
        cost_estimate=pl.CostEstimate(
            flops=12 * HEAD * pairs,
            bytes_accessed=8 * acts.size + 8 * keys.size,
            transcendentals=pairs,
        ),
    )(acts, keys, values, grads, docs, order)


def solution(mesh):
    rows = P("section", "cp", "tp")
    return jax.shard_map(
        on_device,
        mesh=mesh,
        in_specs=(rows, rows, rows, rows, P("section", None), P("section", None)),
        out_specs=(rows, rows, rows, rows),
        check_vma=False,
    )
```

```python
import functools

import jax
import jax.numpy as jnp
from jax import lax
from jax.experimental import pallas as pl
from jax.experimental.pallas import tpu as pltpu
from jax.sharding import PartitionSpec as P

HEAD = 128
DOCS = 8
MESH = pl.DeviceIdType.MESH


def times(a, b, dims):
    return lax.dot_general(a, b, (dims, ((), ())), preferred_element_type=jnp.float32)


def relay_kernel(
    heads, packs, pack, sections, blocks,
    acts, keys, values, grads, docs, order,
    out, gq, gk, gv,
    qbuf, gbuf, kbuf, vbuf, kt, vt, bias, dk, dv, terms, met, held, where_row, doc_row,
    sec_send, sec_recv, kv_send, kv_recv, own_sem, red_send, red_recv, row_sem, token,
):
    scale = HEAD ** (-0.5)
    tok = qbuf.shape[1]
    wide_cols = pack * HEAD
    section = lax.axis_index("section")
    me = lax.axis_index("cp")
    after = lax.rem(section + 1, sections)
    before = lax.rem(section + sections - 1, sections)

    middle = blocks // 2
    offs = sorted(range(1, blocks), key=lambda off: abs(off - middle))

    def peer(off):
        return lax.rem(me + off, blocks)

    rows = (
        pltpu.make_async_copy(order, where_row, row_sem.at[0]),
        pltpu.make_async_copy(docs, doc_row, row_sem.at[1]),
    )
    for row in rows:
        row.start()
    barrier = pltpu.get_barrier_semaphore()
    for where in (after, before):
        pl.semaphore_signal(barrier, inc=1, device_id={"section": where}, device_id_type=MESH)

    @pl.when(me > 0)
    def _():
        pl.semaphore_signal(barrier, inc=1, device_id={"cp": me - 1}, device_id_type=MESH)

    @pl.when(me < blocks - 1)
    def _():
        pl.semaphore_signal(barrier, inc=1, device_id={"cp": me + 1}, device_id_type=MESH)

    pl.semaphore_wait(barrier, 2 + (me + blocks - 1) // blocks + (2 * blocks - 2 - me) // blocks)

    def moved(step, which):
        src, dst, where = ((acts, qbuf, after), (grads, gbuf, before))[which]
        cols = pl.ds(pl.multiple_of(step * wide_cols, wide_cols), wide_cols)
        return pltpu.make_async_remote_copy(
            src_ref=src.at[0, :, cols],
            dst_ref=dst.at[step],
            send_sem=sec_send.at[step, which],
            recv_sem=sec_recv.at[step, which],
            device_id={"section": where},
            device_id_type=MESH,
        )

    def mine(ref, head):
        cols = pl.ds(pl.multiple_of(head * HEAD, HEAD), HEAD)
        return ref.at[0, :, cols]

    own_rows = pl.ds(pl.multiple_of(me * tok, tok), tok)

    def shared(head, which, off):
        src, dst = ((keys, kbuf), (values, vbuf))[which]
        return pltpu.make_async_remote_copy(
            src_ref=mine(src, head),
            dst_ref=dst.at[head, own_rows],
            send_sem=kv_send.at[head, which, off - 1],
            recv_sem=kv_recv.at[head, which, off - 1],
            device_id={"cp": peer(off)},
            device_id_type=MESH,
        )

    def kept(head, which):
        src, dst = ((keys, kbuf), (values, vbuf))[which]
        return pltpu.make_async_copy(
            mine(src, head), dst.at[head, own_rows], own_sem.at[head, which]
        )

    def returned(head, off):
        rows = pl.ds(pl.multiple_of(peer(off) * tok, tok), tok)
        return pltpu.make_async_remote_copy(
            src_ref=terms.at[head, rows],
            dst_ref=met.at[head, off - 1],
            send_sem=red_send.at[head, off - 1],
            recv_sem=red_recv.at[head, off - 1],
            device_id={"cp": peer(off)},
            device_id_type=MESH,
        )

    steps = heads * packs

    @pl.loop(0, steps)
    def _(step):
        for which in range(2):
            moved(step, which).start()

    for side, ahead, behind in ((0, me > 0, me < blocks - 1), (1, me < blocks - 1, me > 0)):
        step_on = me + 1 - 2 * side

        @pl.when(ahead)
        def _():
            pl.semaphore_wait(token.at[side], 1)

        @pl.when(behind)
        def _():
            pl.semaphore_signal(
                token.at[side], inc=1, device_id={"cp": step_on}, device_id_type=MESH
            )

    @pl.loop(0, heads)
    def _(head):
        for which in range(2):
            for off in range(1, blocks):
                shared(head, which, off).start()
            kept(head, which).start()

    for row in rows:
        row.wait()
    positions = where_row[...].astype(jnp.float32)
    asked = where_row[:, own_rows].astype(jnp.float32)
    low = jnp.zeros_like(asked)
    for doc in range(1, DOCS):
        start = jnp.sum(
            jnp.where(doc_row[...] < doc, 1.0, 0.0), axis=1, keepdims=True
        )
        low = jnp.maximum(low, jnp.where(start <= asked, start, 0.0))
    count = positions.shape[1]
    stored = jnp.broadcast_to(positions, (tok, count)).T
    allowed = (stored <= asked) & (stored >= low)
    bias[...] = jnp.where(allowed, 0.0, -1e30)

    def finish(head):
        total = terms[head, own_rows, :].astype(jnp.float32)
        for off in range(1, blocks):
            returned(head, off).wait_recv()
            total = total + met[head, off - 1].astype(jnp.float32)
        cols = pl.ds(pl.multiple_of(head * HEAD, HEAD), HEAD)
        gk[0, :, cols] = total[:, :HEAD].astype(jnp.bfloat16)
        gv[0, :, cols] = total[:, HEAD:].astype(jnp.bfloat16)

    @pl.loop(0, heads)
    def _(head):
        for which in range(2):
            kept(head, which).wait()
            for off in range(1, blocks):
                shared(head, which, off).wait_recv()
        kt[...] = kbuf[head].T
        vt[...] = vbuf[head].T
        dk[...] = jnp.zeros_like(dk)
        dv[...] = jnp.zeros_like(dv)

        def one(step, last):
            for which in range(2):
                moved(step, which).wait_recv()

            parts = [slice(j * HEAD, (j + 1) * HEAD) for j in range(pack)]
            q = jnp.concatenate([qbuf[step, :, c] for c in parts], axis=0)
            g = jnp.concatenate([gbuf[step, :, c] for c in parts], axis=0)
            masked = jnp.concatenate([bias[...]] * pack, axis=1)
            scores = times(kbuf[head], q, ((1,), (1,))) * scale + masked
            expd = jnp.exp(scores - jnp.max(scores, axis=0, keepdims=True))
            probs = (expd * (1.0 / jnp.sum(expd, axis=0, keepdims=True))).astype(jnp.bfloat16)
            dprob = times(vbuf[head], g, ((1,), (1,)))
            wide = probs.astype(jnp.float32)
            delta = jnp.sum(wide * dprob, axis=0, keepdims=True)
            dscore = (wide * (dprob - delta)).astype(jnp.bfloat16)
            dv_now = dv[...] + times(probs, g, ((1,), (0,)))
            dk_now = dk[...] + times(dscore, q, ((1,), (0,)))
            for j in range(pack):
                held[0, j] = probs[:, j * tok : (j + 1) * tok]
                held[1, j] = dscore[:, j * tok : (j + 1) * tok]
            if last:
                terms[head, :, HEAD:] = dv_now.astype(jnp.bfloat16)
                terms[head, :, :HEAD] = (dk_now * scale).astype(jnp.bfloat16)
                for off in offs:
                    returned(head, off).start()
            else:
                dv[...] = dv_now
                dk[...] = dk_now

            @pl.loop(0, pack)
            def _(j):
                attended = times(vt[...], held[0, j], ((1,), (0,))).T
                dquery = times(kt[...], held[1, j], ((1,), (0,))).T
                here = pl.ds(pl.multiple_of(j * HEAD, HEAD), HEAD)
                cols = pl.ds(pl.multiple_of(step * wide_cols + j * HEAD, HEAD), HEAD)
                query = qbuf[step, :, here].astype(jnp.float32)
                cotan = gbuf[step, :, here].astype(jnp.float32)
                out[0, :, cols] = (query + attended).astype(jnp.bfloat16)
                gq[0, :, cols] = (cotan + dquery * scale).astype(jnp.bfloat16)

        @pl.loop(0, packs - 1)
        def _(p):
            one(head * packs + p, False)

        one(head * packs + packs - 1, True)

        @pl.when(head > 0)
        def _():
            finish(head - 1)

    @pl.loop(0, steps)
    def _(step):
        for which in range(2):
            moved(step, which).wait_send()

    @pl.loop(0, heads)
    def _(head):
        for off in range(1, blocks):
            for which in range(2):
                shared(head, which, off).wait_send()

    finish(heads - 1)

    @pl.loop(0, heads)
    def _(head):
        for off in range(1, blocks):
            returned(head, off).wait_send()


def flush_kernel(*refs):
    sem = refs[-1]
    copies = [pltpu.make_async_copy(refs[i], refs[4 + i], sem.at[i]) for i in range(4)]
    for copy in copies:
        copy.start()
    for copy in copies:
        copy.wait()


def on_device(acts, keys, values, grads, docs, order):
    tok = acts.shape[1]
    heads = keys.shape[2] // HEAD
    group = acts.shape[2] // keys.shape[2]
    pack = 2 if group % 2 == 0 else 1
    packs = group // pack
    sections, blocks = lax.axis_size("section"), lax.axis_size("cp")
    count = blocks * tok
    steps = heads * packs
    pairs = group * heads * tok * count
    half, dma = jnp.bfloat16, pltpu.SemaphoreType.DMA
    far = pl.BlockSpec(memory_space=pltpu.HBM)
    near = pl.BlockSpec(memory_space=pltpu.VMEM)
    shapes = tuple(jax.ShapeDtypeStruct(a.shape, half) for a in (acts, acts, keys, keys))
    args = (acts, keys, values, grads, docs, order)
    near_results = pl.pallas_call(
        functools.partial(relay_kernel, heads, packs, pack, sections, blocks),
        out_shape=shapes,
        in_specs=[far] * 6,
        out_specs=(near,) * 4,
        scratch_shapes=[
            pltpu.VMEM((steps, tok, pack * HEAD), half),
            pltpu.VMEM((steps, tok, pack * HEAD), half),
            pltpu.VMEM((heads, count, HEAD), half),
            pltpu.VMEM((heads, count, HEAD), half),
            pltpu.VMEM((HEAD, count), half),
            pltpu.VMEM((HEAD, count), half),
            pltpu.VMEM((count, tok), jnp.float32),
            pltpu.VMEM((count, HEAD), jnp.float32),
            pltpu.VMEM((count, HEAD), jnp.float32),
            pltpu.VMEM((heads, count, 2 * HEAD), half),
            pltpu.VMEM((heads, blocks - 1, tok, 2 * HEAD), half),
            pltpu.VMEM((2, pack, count, tok), half),
            pltpu.VMEM(order.shape, order.dtype),
            pltpu.VMEM(docs.shape, docs.dtype),
            dma((steps, 2)),
            dma((steps, 2)),
            dma((heads, 2, blocks - 1)),
            dma((heads, 2, blocks - 1)),
            dma((heads, 2)),
            dma((heads, blocks - 1)),
            dma((heads, blocks - 1)),
            dma((2,)),
            pltpu.SemaphoreType.REGULAR((2,)),
        ],
        compiler_params=pltpu.CompilerParams(
            collective_id=0,
            has_side_effects=True,
            vmem_limit_bytes=48 * 1024 * 1024,
        ),
        cost_estimate=pl.CostEstimate(
            flops=12 * HEAD * pairs,
            bytes_accessed=8 * acts.size + 8 * keys.size,
            transcendentals=pairs,
        ),
    )(*(pltpu.with_memory_space_constraint(arg, pltpu.HBM) for arg in args))
    return pl.pallas_call(
        flush_kernel,
        out_shape=shapes,
        in_specs=[near] * 4,
        out_specs=(far,) * 4,
        scratch_shapes=[dma((4,))],
        compiler_params=pltpu.CompilerParams(vmem_limit_bytes=8 * 1024 * 1024),
    )(*near_results)


def solution(mesh):
    rows = P("section", "cp", "tp")
    return jax.shard_map(
        on_device,
        mesh=mesh,
        in_specs=(rows, rows, rows, rows, P("section", None), P("section", None)),
        out_specs=(rows, rows, rows, rows),
        check_vma=False,
    )
```

```python
import functools

import jax
import jax.numpy as jnp
from jax import lax
from jax.experimental import pallas as pl
from jax.experimental.pallas import tpu as pltpu
from jax.sharding import PartitionSpec as P

HEAD = 128
DOCS = 8
MESH = pl.DeviceIdType.MESH


def times(a, b, dims):
    return lax.dot_general(a, b, (dims, ((), ())), preferred_element_type=jnp.float32)


def relay_kernel(
    heads, packs, pack, sections, blocks,
    acts, keys, values, grads, docs, order,
    out, gq, gk, gv,
    qbuf, gbuf, kbuf, vbuf, kt, vt, bias, dk, dv, terms, met, held, where_row, doc_row,
    sec_send, sec_recv, kv_send, kv_recv, own_sem, red_send, red_recv, row_sem, token,
):
    scale = HEAD ** (-0.5)
    tok = qbuf.shape[1]
    wide_cols = pack * HEAD
    section = lax.axis_index("section")
    me = lax.axis_index("cp")
    after = lax.rem(section + 1, sections)
    before = lax.rem(section + sections - 1, sections)

    middle = blocks // 2
    offs = sorted(range(1, blocks), key=lambda off: abs(off - middle))

    def peer(off):
        return lax.rem(me + off, blocks)

    rows = (
        pltpu.make_async_copy(order, where_row, row_sem.at[0]),
        pltpu.make_async_copy(docs, doc_row, row_sem.at[1]),
    )
    for row in rows:
        row.start()
    barrier = pltpu.get_barrier_semaphore()
    for where in (after, before):
        pl.semaphore_signal(barrier, inc=1, device_id={"section": where}, device_id_type=MESH)

    @pl.when(me > 0)
    def _():
        pl.semaphore_signal(barrier, inc=1, device_id={"cp": me - 1}, device_id_type=MESH)

    @pl.when(me < blocks - 1)
    def _():
        pl.semaphore_signal(barrier, inc=1, device_id={"cp": me + 1}, device_id_type=MESH)

    pl.semaphore_wait(barrier, 2 + (me + blocks - 1) // blocks + (2 * blocks - 2 - me) // blocks)

    def carried(slot, which, head, cols):
        src, dst, where = ((acts, qbuf, after), (grads, gbuf, before))[which]
        width = qbuf.shape[2]
        first = pl.multiple_of(head * width + cols.start, HEAD)
        return pltpu.make_async_remote_copy(
            src_ref=src.at[0, :, pl.ds(first, cols.size)],
            dst_ref=dst.at[head, :, cols],
            send_sem=sec_send.at[slot, which],
            recv_sem=sec_recv.at[slot, which],
            device_id={"section": where},
            device_id_type=MESH,
        )

    def whole(head, which):
        return carried(head, which, head, pl.ds(0, qbuf.shape[2]))

    def piece(p, which):
        cols = pl.ds(pl.multiple_of(p * wide_cols, wide_cols), wide_cols)
        return carried(heads - 1 + p, which, heads - 1, cols)

    def mine(ref, head):
        cols = pl.ds(pl.multiple_of(head * HEAD, HEAD), HEAD)
        return ref.at[0, :, cols]

    own_rows = pl.ds(pl.multiple_of(me * tok, tok), tok)

    def shared(head, which, off):
        src, dst = ((keys, kbuf), (values, vbuf))[which]
        return pltpu.make_async_remote_copy(
            src_ref=mine(src, head),
            dst_ref=dst.at[head, own_rows],
            send_sem=kv_send.at[head, which, off - 1],
            recv_sem=kv_recv.at[head, which, off - 1],
            device_id={"cp": peer(off)},
            device_id_type=MESH,
        )

    def kept(head, which):
        src, dst = ((keys, kbuf), (values, vbuf))[which]
        return pltpu.make_async_copy(
            mine(src, head), dst.at[head, own_rows], own_sem.at[head, which]
        )

    def returned(head, off):
        rows = pl.ds(pl.multiple_of(peer(off) * tok, tok), tok)
        return pltpu.make_async_remote_copy(
            src_ref=terms.at[head, rows],
            dst_ref=met.at[head, off - 1],
            send_sem=red_send.at[head, off - 1],
            recv_sem=red_recv.at[head, off - 1],
            device_id={"cp": peer(off)},
            device_id_type=MESH,
        )

    @pl.loop(0, heads - 1)
    def _(head):
        for which in range(2):
            whole(head, which).start()

    @pl.loop(0, packs)
    def _(p):
        for which in range(2):
            piece(p, which).start()

    for side, ahead, behind in ((0, me > 0, me < blocks - 1), (1, me < blocks - 1, me > 0)):
        step_on = me + 1 - 2 * side

        @pl.when(ahead)
        def _():
            pl.semaphore_wait(token.at[side], 1)

        @pl.when(behind)
        def _():
            pl.semaphore_signal(
                token.at[side], inc=1, device_id={"cp": step_on}, device_id_type=MESH
            )

    @pl.loop(0, heads)
    def _(head):
        for which in range(2):
            for off in range(1, blocks):
                shared(head, which, off).start()
            kept(head, which).start()

    for row in rows:
        row.wait()
    positions = where_row[...].astype(jnp.float32)
    asked = where_row[:, own_rows].astype(jnp.float32)
    low = jnp.zeros_like(asked)
    for doc in range(1, DOCS):
        start = jnp.sum(
            jnp.where(doc_row[...] < doc, 1.0, 0.0), axis=1, keepdims=True
        )
        low = jnp.maximum(low, jnp.where(start <= asked, start, 0.0))
    count = positions.shape[1]
    stored = jnp.broadcast_to(positions, (tok, count)).T
    allowed = (stored <= asked) & (stored >= low)
    bias[...] = jnp.where(allowed, 0.0, -1e30)

    def finish(head):
        total = terms[head, own_rows, :].astype(jnp.float32)
        for off in range(1, blocks):
            returned(head, off).wait_recv()
            total = total + met[head, off - 1].astype(jnp.float32)
        cols = pl.ds(pl.multiple_of(head * HEAD, HEAD), HEAD)
        gk[0, :, cols] = total[:, :HEAD].astype(jnp.bfloat16)
        gv[0, :, cols] = total[:, HEAD:].astype(jnp.bfloat16)

    @pl.loop(0, heads)
    def _(head):
        for which in range(2):
            kept(head, which).wait()
            for off in range(1, blocks):
                shared(head, which, off).wait_recv()

        @pl.when(head < heads - 1)
        def _():
            for which in range(2):
                whole(head, which).wait_recv()

        kt[...] = kbuf[head].T
        vt[...] = vbuf[head].T
        dk[...] = jnp.zeros_like(dk)
        dv[...] = jnp.zeros_like(dv)

        def one(p, last):
            @pl.when(head == heads - 1)
            def _():
                for which in range(2):
                    piece(p, which).wait_recv()

            parts = [
                pl.ds(pl.multiple_of(p * wide_cols + j * HEAD, HEAD), HEAD) for j in range(pack)
            ]
            q = jnp.concatenate([qbuf[head, :, c] for c in parts], axis=0)
            g = jnp.concatenate([gbuf[head, :, c] for c in parts], axis=0)
            masked = jnp.concatenate([bias[...]] * pack, axis=1)
            scores = times(kbuf[head], q, ((1,), (1,))) * scale + masked
            expd = jnp.exp(scores - jnp.max(scores, axis=0, keepdims=True))
            probs = (expd * (1.0 / jnp.sum(expd, axis=0, keepdims=True))).astype(jnp.bfloat16)
            dprob = times(vbuf[head], g, ((1,), (1,)))
            wide = probs.astype(jnp.float32)
            delta = jnp.sum(wide * dprob, axis=0, keepdims=True)
            dscore = (wide * (dprob - delta)).astype(jnp.bfloat16)
            dv_now = dv[...] + times(probs, g, ((1,), (0,)))
            dk_now = dk[...] + times(dscore, q, ((1,), (0,)))
            for j in range(pack):
                held[0, p, j] = probs[:, j * tok : (j + 1) * tok]
                held[1, p, j] = dscore[:, j * tok : (j + 1) * tok]
            if last:
                terms[head, :, HEAD:] = dv_now.astype(jnp.bfloat16)
                terms[head, :, :HEAD] = (dk_now * scale).astype(jnp.bfloat16)
                for off in offs:
                    returned(head, off).start()
            else:
                dv[...] = dv_now
                dk[...] = dk_now

        @pl.loop(0, packs - 1)
        def _(p):
            one(p, False)

        one(packs - 1, True)

        @pl.loop(0, packs)
        def _(p):
            @pl.loop(0, pack)
            def _(j):
                attended = times(vt[...], held[0, p, j], ((1,), (0,))).T
                dquery = times(kt[...], held[1, p, j], ((1,), (0,))).T
                here = pl.multiple_of(p * wide_cols + j * HEAD, HEAD)
                cols = pl.ds(pl.multiple_of(head * qbuf.shape[2] + here, HEAD), HEAD)
                query = qbuf[head, :, pl.ds(here, HEAD)].astype(jnp.float32)
                cotan = gbuf[head, :, pl.ds(here, HEAD)].astype(jnp.float32)
                out[0, :, cols] = (query + attended).astype(jnp.bfloat16)
                gq[0, :, cols] = (cotan + dquery * scale).astype(jnp.bfloat16)


    @pl.loop(0, heads - 1)
    def _(head):
        for which in range(2):
            whole(head, which).wait_send()

    @pl.loop(0, packs)
    def _(p):
        for which in range(2):
            piece(p, which).wait_send()

    @pl.loop(0, heads)
    def _(head):
        for off in range(1, blocks):
            for which in range(2):
                shared(head, which, off).wait_send()

    @pl.loop(0, heads)
    def _(head):
        finish(head)

    @pl.loop(0, heads)
    def _(head):
        for off in range(1, blocks):
            returned(head, off).wait_send()


def flush_kernel(*refs):
    sem = refs[-1]
    copies = [pltpu.make_async_copy(refs[i], refs[4 + i], sem.at[i]) for i in range(4)]
    for copy in copies:
        copy.start()
    for copy in copies:
        copy.wait()


def on_device(acts, keys, values, grads, docs, order):
    tok = acts.shape[1]
    heads = keys.shape[2] // HEAD
    group = acts.shape[2] // keys.shape[2]
    pack = 2 if group % 2 == 0 else 1
    packs = group // pack
    sections, blocks = lax.axis_size("section"), lax.axis_size("cp")
    count = blocks * tok
    pieces = heads - 1 + packs
    pairs = group * heads * tok * count
    half, dma = jnp.bfloat16, pltpu.SemaphoreType.DMA
    far = pl.BlockSpec(memory_space=pltpu.HBM)
    near = pl.BlockSpec(memory_space=pltpu.VMEM)
    shapes = tuple(jax.ShapeDtypeStruct(a.shape, half) for a in (acts, acts, keys, keys))
    args = (acts, keys, values, grads, docs, order)
    near_results = pl.pallas_call(
        functools.partial(relay_kernel, heads, packs, pack, sections, blocks),
        out_shape=shapes,
        in_specs=[far] * 6,
        out_specs=(near,) * 4,
        scratch_shapes=[
            pltpu.VMEM((heads, tok, group * HEAD), half),
            pltpu.VMEM((heads, tok, group * HEAD), half),
            pltpu.VMEM((heads, count, HEAD), half),
            pltpu.VMEM((heads, count, HEAD), half),
            pltpu.VMEM((HEAD, count), half),
            pltpu.VMEM((HEAD, count), half),
            pltpu.VMEM((count, tok), jnp.float32),
            pltpu.VMEM((count, HEAD), jnp.float32),
            pltpu.VMEM((count, HEAD), jnp.float32),
            pltpu.VMEM((heads, count, 2 * HEAD), half),
            pltpu.VMEM((heads, blocks - 1, tok, 2 * HEAD), half),
            pltpu.VMEM((2, packs, pack, count, tok), half),
            pltpu.VMEM(order.shape, order.dtype),
            pltpu.VMEM(docs.shape, docs.dtype),
            dma((pieces, 2)),
            dma((pieces, 2)),
            dma((heads, 2, blocks - 1)),
            dma((heads, 2, blocks - 1)),
            dma((heads, 2)),
            dma((heads, blocks - 1)),
            dma((heads, blocks - 1)),
            dma((2,)),
            pltpu.SemaphoreType.REGULAR((2,)),
        ],
        compiler_params=pltpu.CompilerParams(
            collective_id=0,
            has_side_effects=True,
            vmem_limit_bytes=48 * 1024 * 1024,
        ),
        cost_estimate=pl.CostEstimate(
            flops=12 * HEAD * pairs,
            bytes_accessed=8 * acts.size + 8 * keys.size,
            transcendentals=pairs,
        ),
    )(*(pltpu.with_memory_space_constraint(arg, pltpu.HBM) for arg in args))
    return pl.pallas_call(
        flush_kernel,
        out_shape=shapes,
        in_specs=[near] * 4,
        out_specs=(far,) * 4,
        scratch_shapes=[dma((4,))],
        compiler_params=pltpu.CompilerParams(vmem_limit_bytes=8 * 1024 * 1024),
    )(*near_results)


def solution(mesh):
    rows = P("section", "cp", "tp")
    return jax.shard_map(
        on_device,
        mesh=mesh,
        in_specs=(rows, rows, rows, rows, P("section", None), P("section", None)),
        out_specs=(rows, rows, rows, rows),
        check_vma=False,
    )
```
